512 devices in a mesh: row: 8 (over y), col: 32 (over z, x), rep: 2 (over core).
Axes of the slice: x: 4, y: 8, z: 8, core: 2. Of those that a mesh axis runs over, the one named last changes fastest.
Arguments:
- gain: float32 [768, 8, 128, 128], P(('row', 'col'), 'rep'), as said below
- coupled_columns: int32 [768, 8], P(('row', 'col')), may hold values from 0 to 767, as said below
- solution: float32 [98304, 512], P(('row', 'col')), may hold values from -6 to 6
- residual: float32 [98304, 512], P(('row', 'col')), may hold values from -6 to 6
- direction: float32 [98304, 512], P(('row', 'col')), may hold values from -6 to 6
Outputs:
- solution_next: float32 [98304, 512], P(('row', 'col'))
- residual_next: float32 [98304, 512], P(('row', 'col'))
- direction_next: float32 [98304, 512], P(('row', 'col'))
The draws below stay inside these ranges and needn't reach their ends.
Inputs may be any that keep to these rules, and one draw needn't show every extreme that they name: `coupled_columns`: each block row i names first its coupled block columns in ascending order (always i - 1, i, i + 1 where inside 0 to 767, some of i - 3, i - 2, i + 2, i + 3, the coupling being symmetric), at most 7 of them, and then fills the remaining slots with i itself; every named column is within 3 of i. The gain matrix assembled from its blocks is symmetric; padding slots hold zero blocks; each diagonal entry exceeds the sum of the absolute values of the other entries of its row by exactly 1.
All inputs are finite; a program needn't handle non-finite values.
Results may differ from the reference program's by a relative error of at most 0.000061.
Values sent between devices are 32-bit elements; how exact they have to be, the bound alone decides.
No kernel may reach another device: no remote copies, remote signals or barrier semaphores. Data moves between devices by JAX's collectives and lax.ppermute only.
A program may use at most 64 MiB of HBM per device.

```python
import jax
import jax.numpy as jnp
from jax import lax

BLK = 128
SNAP = 512
NB = 768
NS = 98304


reach_blocks = 3


def coupling_layout(key):
    coupling_bits = jax.random.randint(jax.random.fold_in(key, 11), (2, NB), 0, 2).astype(jnp.int32)
    positions = jnp.arange(NB, dtype=jnp.int32)
    offsets = jnp.arange(-reach_blocks, reach_blocks + 1, dtype=jnp.int32)
    targets = positions[:, None] + offsets[None, :]
    inside = jnp.logical_and(targets >= 0, targets < NB)
    always = jnp.ones((NB,), jnp.int32)
    chosen = jnp.stack([jnp.roll(coupling_bits[1], 3), jnp.roll(coupling_bits[0], 2), always, always, always, coupling_bits[0], coupling_bits[1]], axis=1)
    present = jnp.logical_and(inside, chosen == 1)
    slot_keys = jnp.where(present, 0, 16) + offsets[None, :] + reach_blocks
    ordering = jnp.argsort(slot_keys, axis=1, stable=True).astype(jnp.int32)
    present_sorted = jnp.take_along_axis(present, ordering, axis=1)
    targets_sorted = jnp.take_along_axis(targets, ordering, axis=1)
    columns = jnp.where(present_sorted, targets_sorted, positions[:, None])
    columns = jnp.concatenate([columns, positions[:, None]], axis=1).astype(jnp.int32)
    return (present, ordering, columns)


def draw_coupled_columns(key, part):
    present, ordering, columns = coupling_layout(key)
    return columns


def draw_gain(key, part):
    present, ordering, columns = coupling_layout(key)
    spread_scale = (7.0 * BLK) ** (-0.5)
    pair_key = jax.random.fold_in(key, 23)
    own_key = jax.random.fold_in(key, 29)
    pair_noise = jax.random.normal(pair_key, (3, NB, BLK, BLK), jnp.float32) * spread_scale
    own_noise = jax.random.normal(own_key, (NB, BLK, BLK), jnp.float32) * spread_scale
    identity = jnp.eye(BLK, dtype=jnp.float32)
    own_noise = (own_noise + jnp.transpose(own_noise, (0, 2, 1))) * 0.5 * (1.0 - identity)[None]
    upper_blocks = [pair_noise[0], pair_noise[1], pair_noise[2]]
    lower_blocks = [jnp.transpose(jnp.roll(pair_noise[step], step + 1, axis=0), (0, 2, 1)) for step in range(3)]
    stacked = jnp.stack([lower_blocks[2], lower_blocks[1], lower_blocks[0], own_noise, upper_blocks[0], upper_blocks[1], upper_blocks[2]], axis=1)
    stacked = stacked * present[:, :, None, None].astype(jnp.float32)
    dominant = 1.0 + jnp.sum(jnp.abs(stacked), axis=(1, 3))
    diagonal_block = stacked[:, 3] + identity[None] * dominant[:, :, None]
    stacked = stacked.at[:, 3].set(diagonal_block)
    sorted_blocks = jnp.take_along_axis(stacked, ordering[:, :, None, None], axis=1)
    padding = jnp.zeros((NB, 1, BLK, BLK), jnp.float32)
    return jnp.concatenate([sorted_blocks, padding], axis=1)


def shard_levels(key, shape, shards, low, top_value):
    level, own = 1.0, jax.random.fold_in(key, 6)
    for axis_at, shards_of in shards:
        steps = jnp.exp(jax.random.uniform(jax.random.fold_in(own, axis_at), (shards_of,), jnp.float32, low / len(shards), top_value / len(shards)))
        level = level * jnp.repeat(steps, shape[axis_at] // shards_of).reshape([-1 if axis == axis_at else 1 for axis in range(len(shape))])
    return level


def gaussian(key, dims, deviation, reach, shards=(), kind=jnp.bfloat16):
    array = deviation * jax.random.normal(key, dims, jnp.float32)
    if shards:
        array = array * shard_levels(key, dims, shards, -0.22, 0.18)
    return jnp.clip(array, -reach, reach).astype(kind)


def setup_inputs(seed: int = 0) -> dict:
    key_list = jax.random.split(jax.random.key(seed), 6)
    return {
        "gain": draw_gain(jax.random.fold_in(key_list[5], 71), 0),
        "coupled_columns": draw_coupled_columns(jax.random.fold_in(key_list[5], 71), 0),
        "solution": gaussian(key_list[2], (NS, SNAP), 1.0, 6.0, ((0, 256),), jnp.float32),
        "residual": gaussian(key_list[3], (NS, SNAP), 1.0, 6.0, ((0, 256),), jnp.float32),
        "direction": gaussian(key_list[4], (NS, SNAP), 1.0, 6.0, ((0, 256),), jnp.float32),
    }


def reference(gain, coupled_columns, solution, residual, direction):
    snapshots = direction.shape[1]
    segments = direction.reshape(NB, BLK, snapshots)

    def one_row(block_row):
        blocks = gain[block_row]
        picked = segments[coupled_columns[block_row]]
        return jnp.einsum("kab,kbs->as", blocks, picked, precision=lax.Precision.HIGHEST, preferred_element_type=jnp.float32)

    image = lax.map(one_row, jnp.arange(NB, dtype=jnp.int32)).reshape(NS, snapshots)
    norm_old = jnp.sum(residual * residual, axis=0)
    curvature = jnp.sum(direction * image, axis=0)
    step_size = norm_old / curvature
    solution_next = solution + step_size * direction
    residual_next = residual - step_size * image
    norm_new = jnp.sum(residual_next * residual_next, axis=0)
    direction_next = residual_next + (norm_new / norm_old) * direction
    return solution_next, residual_next, direction_next
```

```python
import jax
import jax.numpy as jnp
from jax import lax
from jax.sharding import Mesh
from jax.sharding import PartitionSpec as P

BLK = 128
REACH = 3
ROW_COL = ("row", "col_0", "col_1")
ALL = ("row", "col_0", "col_1", "rep")


def halo_pairs(groups, step):
    pairs = []
    for p in range(groups):
        for rep, to in ((0, p + step), (1, p - step)):
            if 0 <= to < groups:
                pairs.append((2 * p + rep, 2 * to + rep))
    return pairs


def from_all(x, axes, count):
    return lax.all_to_all(jnp.broadcast_to(x[None], (count, *x.shape)), axes, 0, 0, tiled=True)


def per_device(gain, coupled_columns, solution, residual, direction):
    rows = coupled_columns.shape[0]
    snapshots = direction.shape[1]
    half = snapshots // 2
    rep = lax.axis_index("rep")
    groups = lax.axis_size(ROW_COL)
    first_block = lax.axis_index(ROW_COL) * rows

    own = lax.dynamic_slice_in_dim(direction, rep * half, half, axis=1)
    one = lax.ppermute(own, ALL, halo_pairs(groups, 1))
    two = lax.ppermute(own, ALL, halo_pairs(groups, -1))
    other_gain = lax.ppermute(gain, "rep", [(0, 1), (1, 0)])
    res = lax.dynamic_slice_in_dim(residual, rep * half, half, axis=1)

    low = jnp.where(rep == 0, one, two)
    high = jnp.where(rep == 0, two, one)
    segments = jnp.concatenate([low, own, high], axis=0).reshape(rows + 2 * REACH, BLK, half)
    slots = gain.shape[1]
    mine = lax.dynamic_slice_in_dim(coupled_columns, rep * slots, slots, axis=1)
    theirs = lax.dynamic_slice_in_dim(coupled_columns, (1 - rep) * slots, slots, axis=1)
    shift = REACH - first_block
    image = jnp.einsum(
        "rkab,rkbs->ras",
        jnp.concatenate([gain, other_gain], axis=1),
        segments[jnp.concatenate([mine, theirs], axis=1) + shift],
        precision=lax.Precision.HIGHEST,
        preferred_element_type=jnp.float32,
    ).reshape(rows * BLK, half)
    other_image = lax.ppermute(image, "rep", [(0, 1), (1, 0)])

    sums = jnp.stack(
        [
            jnp.sum(res * res, axis=0),
            jnp.sum(own * image, axis=0),
            jnp.sum(res * image, axis=0),
            jnp.sum(image * image, axis=0),
        ]
    ).reshape(8, -1)
    n1 = lax.axis_size("row") * lax.axis_size("col_1")
    sums = jnp.sum(from_all(sums, ("row", "col_1"), n1).reshape(n1, *sums.shape), axis=0)
    n2 = lax.axis_size("col_0")
    sums = jnp.sum(from_all(sums, ("col_0", "rep"), 2 * n2).reshape(n2, 2, *sums.shape), axis=0)
    sums = jnp.concatenate([sums[0].reshape(4, half), sums[1].reshape(4, half)], axis=1)
    norm_old, curvature, crossing, image_square = sums

    left = jnp.where(rep == 0, image, other_image)
    right = jnp.where(rep == 0, other_image, image)
    image = jnp.concatenate([left, right], axis=1)
    step_size = norm_old / curvature
    solution_next = solution + step_size * direction
    residual_next = residual - step_size * image
    norm_new = norm_old - 2.0 * step_size * crossing + step_size * step_size * image_square
    direction_next = residual_next + norm_new / norm_old * direction
    return (solution_next, residual_next, direction_next)


def solution(mesh):
    finer = Mesh(
        mesh.devices.reshape(mesh.shape["row"], 8, 4, mesh.shape["rep"]),
        ALL,
    )
    return jax.shard_map(
        per_device,
        mesh=finer,
        in_specs=(
            P(ROW_COL, "rep", None, None),
            P(ROW_COL, None),
            P(ROW_COL, None),
            P(ROW_COL, None),
            P(ROW_COL, None),
        ),
        out_specs=(P(ROW_COL, None), P(ROW_COL, None), P(ROW_COL, None)),
        check_vma=False,
    )
```

```python
import jax
import jax.numpy as jnp
from jax import lax
from jax.experimental import pallas as pl
from jax.experimental.pallas import tpu as pltpu
from jax.sharding import Mesh
from jax.sharding import PartitionSpec as P

BLK = 128
REACH = 3
CHUNKS = 4
ROW_COL = ("row", "col_0", "col_1")
ALL = ("row", "col_0", "col_1", "rep")
F32, BF16 = jnp.float32, jnp.bfloat16


def halo_pairs(groups, first):
    pairs = []
    for rep in range(2):
        for p in range((rep + 1 - first) % 2, groups - 1, 2):
            near, far = 2 * p + rep, 2 * (p + 1) + rep
            pairs += [(near, far), (far, near)]
    return pairs


def split(x):
    top = x.astype(BF16)
    return top, (x - top.astype(F32)).astype(BF16)


def dot3(a_top, a_rest, x):
    x_top, x_rest = split(x)
    dot = lambda a, b: jnp.dot(a, b, preferred_element_type=F32)
    return dot(a_top, x_top) + (dot(a_top, x_rest) + dot(a_rest, x_top))


def place_blocks(columns, blocks, offset, dense):
    rows, slots = blocks.shape[0], blocks.shape[1]
    segment = lax.axis_index(ROW_COL)
    low_first = (segment + lax.axis_index("rep")) % 2 == 1
    for i in range(rows):
        for k in range(slots):
            w = columns[i, offset + k] - segment * rows + REACH
            low = jnp.where(low_first, w, w + 3)
            high = jnp.where(low_first, w - 3, w - 6)
            c = jnp.where(w < 3, low, jnp.where(w > 5, high, w + 3))
            here = pl.ds(i * BLK, BLK)
            dense[c, here, :] = dense[c, here, :] + blocks[i, k]


def begin(columns, gain, residual, direction, solution, dense, norm):
    rep = lax.axis_index("rep")
    half = residual.shape[1] // 2
    dense[...] = jnp.zeros_like(dense)
    place_blocks(columns, gain, rep * gain.shape[1], dense)
    r = residual[:, pl.ds(pl.multiple_of(rep * half, half), half)]
    norm[...] = jnp.sum(r * r, axis=0, keepdims=True)


def prepare(columns, other, own, start, top, rest, local, dense):
    dense[...] = start[...]
    place_blocks(columns, other, (1 - lax.axis_index("rep")) * other.shape[1], dense)
    for c in range(6):
        top[c], rest[c] = split(dense[c])
    middle = jnp.concatenate([dense[6], dense[7], dense[8]], axis=1)
    m_top, m_rest = split(middle)
    local[...] = dot3(m_top, m_rest, own[...])


def finish(one, two, top, rest, local, own, res, norm, image, sums):
    x = jnp.concatenate([one[...], two[...]], axis=0)
    product = local[...]
    half = product.shape[1]
    for pair in range(3):
        a_top = jnp.concatenate([top[2 * pair], top[2 * pair + 1]], axis=1)
        a_rest = jnp.concatenate([rest[2 * pair], rest[2 * pair + 1]], axis=1)
        product += dot3(a_top, a_rest, x[2 * pair * BLK : 2 * (pair + 1) * BLK])
    image[...] = product
    r = res[:, pl.ds(pl.multiple_of(lax.axis_index("rep") * half, half), half)]
    rows = [
        norm[...],
        jnp.sum(own[...] * product, axis=0, keepdims=True),
        jnp.sum(r * product, axis=0, keepdims=True),
        jnp.sum(product * product, axis=0, keepdims=True),
    ]
    packed = jnp.concatenate([v[:, h : h + BLK] for v in rows for h in range(0, half, BLK)], axis=0)
    sums[...] = jnp.broadcast_to(packed[None], sums.shape)


def fold(terms, sums):
    sums[...] = jnp.broadcast_to(jnp.sum(terms[...], axis=0)[None], sums.shape)


def update(terms, image, other, solution, residual, direction, sol_next, res_next, dir_next):
    half = image.shape[1]
    chunk = sol_next.shape[0]
    rep = lax.axis_index("rep")
    here = pl.ds(pl.multiple_of(pl.program_id(0) * chunk, chunk), chunk)
    for side in range(2):
        total = terms[side]
        for n in range(1, terms.shape[0] // 2):
            total += terms[2 * n + side]
        mine = rep == side
        for h in range(half // BLK):
            lanes = slice(side * half + h * BLK, side * half + (h + 1) * BLK)
            part = slice(h * BLK, (h + 1) * BLK)
            norm_old, curvature, crossing, square = (total[2 * n + h : 2 * n + h + 1] for n in range(4))
            step = norm_old / curvature
            norm_new = norm_old - 2.0 * step * crossing + step * step * square
            ratio = norm_new / norm_old
            product = jnp.where(mine, image[here, part], other[here, part])
            d = direction[here, lanes]
            sol_next[:, lanes] = solution[here, lanes] + step * d
            r = residual[here, lanes] - step * product
            res_next[:, lanes] = r
            dir_next[:, lanes] = r + ratio * d


def vmem(n):
    return [pl.BlockSpec(memory_space=pltpu.VMEM)] * n


def from_all(x, axes):
    return lax.all_to_all(x, axes, 0, 0, tiled=True)


def iteration(gain, coupled_columns, solution, residual, direction):
    rows, _ = gain.shape[:2]
    states, snapshots = direction.shape
    half = snapshots // 2
    rep = lax.axis_index("rep")
    groups = lax.axis_size(ROW_COL)

    own = lax.dynamic_slice_in_dim(direction, rep * half, half, axis=1)
    one = lax.ppermute(own, ALL, halo_pairs(groups, True))
    two = lax.ppermute(own, ALL, halo_pairs(groups, False))
    other_gain = lax.ppermute(gain, "rep", [(0, 1), (1, 0)])
    smem = pl.BlockSpec(memory_space=pltpu.SMEM)
    halves = jax.ShapeDtypeStruct((states, half), F32)
    whole = jax.ShapeDtypeStruct((states, snapshots), F32)
    terms = jax.ShapeDtypeStruct((2 * rows, states, BLK), BF16)
    band = jax.ShapeDtypeStruct((3 * rows, states, BLK), F32)
    dense, norm = pl.pallas_call(
        begin,
        out_shape=(band, jax.ShapeDtypeStruct((1, half), F32)),
        in_specs=[smem, *vmem(4)],
        out_specs=tuple(vmem(2)),
        cost_estimate=pl.CostEstimate(flops=4_000_000, bytes_accessed=5_000_000, transcendentals=0),
        compiler_params=pltpu.CompilerParams(vmem_limit_bytes=10 << 20),
        name="begin",
    )(coupled_columns, gain, residual, direction, solution)
    top, rest, local = pl.pallas_call(
        prepare,
        out_shape=(terms, terms, halves),
        in_specs=[smem, *vmem(3)],
        out_specs=tuple(vmem(3)),
        scratch_shapes=[pltpu.VMEM(band.shape, F32)],
        cost_estimate=pl.CostEstimate(flops=400_000_000, bytes_accessed=5_000_000, transcendentals=0),
        compiler_params=pltpu.CompilerParams(vmem_limit_bytes=10 << 20),
        name="prepare",
    )(coupled_columns, other_gain, own, dense)

    n1 = lax.axis_size("row") * lax.axis_size("col_1")
    n2 = 2 * lax.axis_size("col_0")
    image, sums = pl.pallas_call(
        finish,
        out_shape=(halves, jax.ShapeDtypeStruct((n1, 8, BLK), F32)),
        in_specs=vmem(8),
        out_specs=tuple(vmem(2)),
        cost_estimate=pl.CostEstimate(flops=500_000_000, bytes_accessed=5_000_000, transcendentals=0),
        compiler_params=pltpu.CompilerParams(vmem_limit_bytes=10 << 20),
        name="finish",
    )(one, two, top, rest, local, own, residual, norm)
    sums = from_all(sums, ("row", "col_1"))
    sums = pl.pallas_call(
        fold,
        out_shape=jax.ShapeDtypeStruct((n2, 8, BLK), F32),
        in_specs=vmem(1),
        out_specs=vmem(1)[0],
        compiler_params=pltpu.CompilerParams(vmem_limit_bytes=2 << 20),
        name="fold",
    )(sums)
    image, sums = lax.optimization_barrier((image, sums))
    other_image = lax.ppermute(image, "rep", [(0, 1), (1, 0)])
    sums = from_all(sums, ("col_0", "rep"))

    chunk = states // CHUNKS
    block = pl.BlockSpec((chunk, snapshots), lambda c: (c, 0))
    return pl.pallas_call(
        update,
        grid=(CHUNKS,),
        out_shape=(whole, whole, whole),
        in_specs=vmem(6),
        out_specs=(block, block, block),
        compiler_params=pltpu.CompilerParams(vmem_limit_bytes=10 << 20),
        name="update",
    )(sums, image, other_image, solution, residual, direction)


def solution(mesh):
    finer = Mesh(
        mesh.devices.reshape(mesh.shape["row"], 8, 4, mesh.shape["rep"]),
        ALL,
    )
    return jax.shard_map(
        iteration,
        mesh=finer,
        in_specs=(
            P(ROW_COL, "rep", None, None),
            P(ROW_COL, None),
            P(ROW_COL, None),
            P(ROW_COL, None),
            P(ROW_COL, None),
        ),
        out_specs=(P(ROW_COL, None), P(ROW_COL, None), P(ROW_COL, None)),
        check_vma=False,
    )
```

```python
import jax
import jax.numpy as jnp
from jax import lax
from jax.experimental import pallas as pl
from jax.experimental.pallas import tpu as pltpu
from jax.sharding import Mesh
from jax.sharding import PartitionSpec as P

BLK = 128
REACH = 3
CHUNKS = 2
ROW_COL = ("row", "col_0", "col_1")
ALL = ("row", "col_0", "col_1", "rep")
F32, BF16 = jnp.float32, jnp.bfloat16


def halo_pairs(groups, first):
    pairs = []
    for rep in range(2):
        for p in range((rep + 1 - first) % 2, groups - 1, 2):
            near, far = 2 * p + rep, 2 * (p + 1) + rep
            pairs += [(near, far), (far, near)]
    return pairs


def split(x):
    top = x.astype(BF16)
    return top, (x - top.astype(F32)).astype(BF16)


def dot3(a_top, a_rest, x):
    x_top, x_rest = split(x)
    dot = lambda a, b: jnp.dot(a, b, preferred_element_type=F32)
    return dot(a_top, x_top) + (dot(a_top, x_rest) + dot(a_rest, x_top))


def take_half(direction, own, sem):
    half = own.shape[1]
    at = pl.ds(pl.multiple_of(lax.axis_index("rep") * half, half), half)
    copy = pltpu.make_async_copy(direction.at[:, at], own, sem)
    copy.start()
    copy.wait()


def place_blocks(columns, blocks, offset, dense):
    rows, slots = blocks.shape[0], blocks.shape[1]
    segment = lax.axis_index(ROW_COL)
    low_first = (segment + lax.axis_index("rep")) % 2 == 1
    for i in range(rows):
        for k in range(slots):
            w = columns[i, offset + k] - segment * rows + REACH
            low = jnp.where(low_first, w, w + 3)
            high = jnp.where(low_first, w - 3, w - 6)
            c = jnp.where(w < 3, low, jnp.where(w > 5, high, w + 3))
            here = pl.ds(i * BLK, BLK)
            dense[c, here, :] = dense[c, here, :] + blocks[i, k]


def begin(columns, gain, residual, direction, solution, dense, norm, res, dir_, sol, mine, sems):
    rep = lax.axis_index("rep")
    half = residual.shape[1] // 2
    ends = ((gain, mine), (residual, res), (direction, dir_), (solution, sol))
    copies = [pltpu.make_async_copy(*pair, sems.at[n]) for n, pair in enumerate(ends)]
    for copy in copies:
        copy.start()
    dense[...] = jnp.zeros_like(dense)
    copies[0].wait()
    place_blocks(columns, mine, rep * mine.shape[1], dense)
    copies[1].wait()
    r = res[:, pl.ds(pl.multiple_of(rep * half, half), half)]
    norm[...] = jnp.sum(r * r, axis=0, keepdims=True)
    copies[2].wait()
    copies[3].wait()


def prepare(columns, other, own, start, top_1, rest_1, top_2, rest_2, local, dense):
    dense[...] = start[...]
    place_blocks(columns, other, (1 - lax.axis_index("rep")) * other.shape[1], dense)
    for c in range(3):
        top_1[c], rest_1[c] = split(dense[c])
        top_2[c], rest_2[c] = split(dense[3 + c])
    middle = jnp.concatenate([dense[6], dense[7], dense[8]], axis=1)
    m_top, m_rest = split(middle)
    local[...] = dot3(m_top, m_rest, own[...])


def add_halo(start, x, top, rest):
    join = lambda terms: jnp.concatenate([terms[c] for c in range(3)], axis=1)
    return start[...] + dot3(join(top), join(rest), x[...])


def first_halo(one, top, rest, local, partial):
    partial[...] = add_halo(local, one, top, rest)


def finish(two, top, rest, partial, own, res, norm, image, sums):
    product = add_halo(partial, two, top, rest)
    half = product.shape[1]
    image[...] = product
    r = res[:, pl.ds(pl.multiple_of(lax.axis_index("rep") * half, half), half)]
    rows = [
        norm[...],
        jnp.sum(own[...] * product, axis=0, keepdims=True),
        jnp.sum(r * product, axis=0, keepdims=True),
        jnp.sum(product * product, axis=0, keepdims=True),
    ]
    packed = jnp.concatenate([v[:, h : h + BLK] for v in rows for h in range(0, half, BLK)], axis=0)
    sums[...] = jnp.broadcast_to(packed[None], sums.shape)


def fold(terms, sums):
    sums[...] = jnp.broadcast_to(jnp.sum(terms[...], axis=0)[None], sums.shape)


def update(terms, image, other, solution, residual, direction, sol_next, res_next, dir_next):
    half = image.shape[1]
    chunk = sol_next.shape[0]
    rep = lax.axis_index("rep")
    here = pl.ds(pl.multiple_of(pl.program_id(0) * chunk, chunk), chunk)
    for side in range(2):
        total = terms[side]
        for n in range(1, terms.shape[0] // 2):
            total += terms[2 * n + side]
        mine = rep == side
        for h in range(half // BLK):
            lanes = slice(side * half + h * BLK, side * half + (h + 1) * BLK)
            part = slice(h * BLK, (h + 1) * BLK)
            norm_old, curvature, crossing, square = (total[2 * n + h : 2 * n + h + 1] for n in range(4))
            step = norm_old / curvature
            norm_new = norm_old - 2.0 * step * crossing + step * step * square
            ratio = norm_new / norm_old
            product = jnp.where(mine, image[here, part], other[here, part])
            d = direction[here, lanes]
            sol_next[:, lanes] = solution[here, lanes] + step * d
            r = residual[here, lanes] - step * product
            res_next[:, lanes] = r
            dir_next[:, lanes] = r + ratio * d


def in_hbm(x):
    return pltpu.with_memory_space_constraint(x, pltpu.HBM)


def vmem(n):
    return [pl.BlockSpec(memory_space=pltpu.VMEM)] * n


def from_all(x, axes):
    return lax.all_to_all(x, axes, 0, 0, tiled=True)


def iteration(gain, coupled_columns, solution, residual, direction):
    rows, _ = gain.shape[:2]
    states, snapshots = direction.shape
    half = snapshots // 2
    groups = lax.axis_size(ROW_COL)

    halves = jax.ShapeDtypeStruct((states, half), F32)
    own = pl.pallas_call(
        take_half,
        out_shape=halves,
        in_specs=[pl.BlockSpec(memory_space=pltpu.HBM)],
        out_specs=vmem(1)[0],
        scratch_shapes=[pltpu.SemaphoreType.DMA],
        compiler_params=pltpu.CompilerParams(vmem_limit_bytes=2 << 20),
        name="take_half",
    )(in_hbm(direction))
    one = lax.ppermute(own, ALL, halo_pairs(groups, True))
    two = lax.ppermute(own, ALL, halo_pairs(groups, False))
    other_gain = lax.ppermute(gain, "rep", [(0, 1), (1, 0)])
    smem = pl.BlockSpec(memory_space=pltpu.SMEM)
    whole = jax.ShapeDtypeStruct((states, snapshots), F32)
    terms = jax.ShapeDtypeStruct((REACH, states, BLK), BF16)
    band = jax.ShapeDtypeStruct((3 * rows, states, BLK), F32)
    dense, norm, res, dir_, sol = pl.pallas_call(
        begin,
        out_shape=(band, jax.ShapeDtypeStruct((1, half), F32), whole, whole, whole),
        in_specs=[smem, *[pl.BlockSpec(memory_space=pltpu.HBM)] * 4],
        out_specs=tuple(vmem(5)),
        scratch_shapes=[pltpu.VMEM(gain.shape, F32), pltpu.SemaphoreType.DMA((4,))],
        cost_estimate=pl.CostEstimate(flops=4_000_000, bytes_accessed=5_000_000, transcendentals=0),
        compiler_params=pltpu.CompilerParams(vmem_limit_bytes=12 << 20),
        name="begin",
    )(in_hbm(coupled_columns), *map(in_hbm, (gain, residual, direction, solution)))
    *terms, local = pl.pallas_call(
        prepare,
        out_shape=(*[terms] * 4, halves),
        in_specs=[smem, *vmem(3)],
        out_specs=tuple(vmem(5)),
        scratch_shapes=[pltpu.VMEM(band.shape, F32)],
        cost_estimate=pl.CostEstimate(flops=400_000_000, bytes_accessed=5_000_000, transcendentals=0),
        compiler_params=pltpu.CompilerParams(vmem_limit_bytes=10 << 20),
        name="prepare",
    )(in_hbm(coupled_columns), other_gain, own, dense)

    n1 = lax.axis_size("row") * lax.axis_size("col_1")
    n2 = 2 * lax.axis_size("col_0")
    partial = pl.pallas_call(
        first_halo,
        out_shape=halves,
        in_specs=vmem(4),
        out_specs=vmem(1)[0],
        cost_estimate=pl.CostEstimate(flops=250_000_000, bytes_accessed=1_000_000, transcendentals=0),
        compiler_params=pltpu.CompilerParams(vmem_limit_bytes=8 << 20),
        name="first_halo",
    )(one, terms[0], terms[1], local)
    image, sums = pl.pallas_call(
        finish,
        out_shape=(halves, jax.ShapeDtypeStruct((n1, 8, BLK), F32)),
        in_specs=vmem(7),
        out_specs=tuple(vmem(2)),
        cost_estimate=pl.CostEstimate(flops=500_000_000, bytes_accessed=5_000_000, transcendentals=0),
        compiler_params=pltpu.CompilerParams(vmem_limit_bytes=10 << 20),
        name="finish",
    )(two, terms[2], terms[3], partial, own, res, norm)
    sums = from_all(sums, ("row", "col_1"))
    other_image = lax.ppermute(image, "rep", [(0, 1), (1, 0)])
    sums = pl.pallas_call(
        fold,
        out_shape=jax.ShapeDtypeStruct((n2, 8, BLK), F32),
        in_specs=vmem(1),
        out_specs=vmem(1)[0],
        compiler_params=pltpu.CompilerParams(vmem_limit_bytes=2 << 20),
        name="fold",
    )(sums)
    sums = from_all(sums, ("col_0", "rep"))

    chunk = states // CHUNKS
    block = pl.BlockSpec((chunk, snapshots), lambda c: (c, 0))
    return pl.pallas_call(
        update,
        grid=(CHUNKS,),
        out_shape=(whole, whole, whole),
        in_specs=vmem(6),
        out_specs=(block, block, block),
        compiler_params=pltpu.CompilerParams(vmem_limit_bytes=10 << 20),
        name="update",
    )(sums, image, other_image, sol, res, dir_)


def solution(mesh):
    finer = Mesh(
        mesh.devices.reshape(mesh.shape["row"], 8, 4, mesh.shape["rep"]),
        ALL,
    )
    return jax.shard_map(
        iteration,
        mesh=finer,
        in_specs=(
            P(ROW_COL, "rep", None, None),
            P(ROW_COL, None),
            P(ROW_COL, None),
            P(ROW_COL, None),
            P(ROW_COL, None),
        ),
        out_specs=(P(ROW_COL, None), P(ROW_COL, None), P(ROW_COL, None)),
        check_vma=False,
    )
```

```python
import jax
import jax.numpy as jnp
from jax import lax
from jax.experimental import pallas as pl
from jax.experimental.pallas import tpu as pltpu
from jax.sharding import Mesh
from jax.sharding import PartitionSpec as P

BLK = 128
REACH = 3
CHUNKS = 2
ROW_COL = ("row", "col_0", "col_1")
ALL = ("row", "col_0", "col_1", "rep")
F32, BF16 = jnp.float32, jnp.bfloat16


def halo_pairs(groups, first):
    pairs = []
    for rep in range(2):
        for p in range((rep + 1 - first) % 2, groups - 1, 2):
            near, far = 2 * p + rep, 2 * (p + 1) + rep
            pairs += [(near, far), (far, near)]
    return pairs


def split(x):
    top = x.astype(BF16)
    return top, (x - top.astype(F32)).astype(BF16)


def dot3(a_top, a_rest, x):
    x_top, x_rest = split(x)
    dot = lambda a, b: jnp.dot(a, b, preferred_element_type=F32)
    return dot(a_top, x_top) + (dot(a_top, x_rest) + dot(a_rest, x_top))


def take_half(direction, own, sem):
    half = own.shape[1]
    at = pl.ds(pl.multiple_of(lax.axis_index("rep") * half, half), half)
    copy = pltpu.make_async_copy(direction.at[:, at], own, sem)
    copy.start()
    copy.wait()


def place_blocks(columns, blocks, offset, dense):
    rows, slots = blocks.shape[0], blocks.shape[1]
    segment = lax.axis_index(ROW_COL)
    low_first = (segment + lax.axis_index("rep")) % 2 == 1
    for i in range(rows):
        for k in range(slots):
            w = columns[i, offset + k] - segment * rows + REACH
            low = jnp.where(low_first, w, w + 3)
            high = jnp.where(low_first, w - 3, w - 6)
            c = jnp.where(w < 3, low, jnp.where(w > 5, high, w + 3))
            here = pl.ds(i * BLK, BLK)
            dense[c, here, :] = dense[c, here, :] + blocks[i, k]


def begin(columns, gain, residual, direction, solution, dense, norm, res, dir_, sol, mine, sems):
    rep = lax.axis_index("rep")
    half = residual.shape[1] // 2
    ends = ((gain, mine), (residual, res), (direction, dir_), (solution, sol))
    copies = [pltpu.make_async_copy(*pair, sems.at[n]) for n, pair in enumerate(ends)]
    for copy in copies:
        copy.start()
    dense[...] = jnp.zeros_like(dense)
    copies[0].wait()
    place_blocks(columns, mine, rep * mine.shape[1], dense)
    copies[1].wait()
    r = res[:, pl.ds(pl.multiple_of(rep * half, half), half)]
    norm[...] = jnp.sum(r * r, axis=0, keepdims=True)
    copies[2].wait()
    copies[3].wait()


def prepare(columns, other, own, start, top_1, rest_1, top_2, rest_2, local, dense):
    dense[...] = start[...]
    place_blocks(columns, other, (1 - lax.axis_index("rep")) * other.shape[1], dense)
    for c in range(3):
        top_1[c], rest_1[c] = split(dense[c])
        top_2[c], rest_2[c] = split(dense[3 + c])
    middle = jnp.concatenate([dense[6], dense[7], dense[8]], axis=1)
    m_top, m_rest = split(middle)
    local[...] = dot3(m_top, m_rest, own[...])


def add_halo(start, x, top, rest):
    join = lambda terms: jnp.concatenate([terms[c] for c in range(3)], axis=1)
    return start[...] + dot3(join(top), join(rest), x[...])


def first_halo(one, top, rest, local, partial):
    partial[...] = add_halo(local, one, top, rest)


def finish(two, top, rest, partial, own, res, norm, image, sums):
    product = add_halo(partial, two, top, rest)
    half = product.shape[1]
    image[...] = product
    r = res[:, pl.ds(pl.multiple_of(lax.axis_index("rep") * half, half), half)]
    rows = [
        norm[...],
        jnp.sum(own[...] * product, axis=0, keepdims=True),
        jnp.sum(r * product, axis=0, keepdims=True),
        jnp.sum(product * product, axis=0, keepdims=True),
    ]
    packed = jnp.concatenate([v[:, h : h + BLK] for v in rows for h in range(0, half, BLK)], axis=0)
    sums[...] = jnp.broadcast_to(packed[None], sums.shape)


def fold(terms, sums):
    sums[...] = jnp.broadcast_to(jnp.sum(terms[...], axis=0)[None], sums.shape)


def update(terms, image, other, solution, residual, direction, sol_next, res_next, dir_next):
    half = image.shape[1]
    chunk = sol_next.shape[0]
    rep = lax.axis_index("rep")
    here = pl.ds(pl.multiple_of(pl.program_id(0) * chunk, chunk), chunk)
    for side in range(2):
        count = terms.shape[0] // 2
        total = terms[side * count]
        for n in range(1, count):
            total += terms[side * count + n]
        mine = rep == side
        for h in range(half // BLK):
            lanes = slice(side * half + h * BLK, side * half + (h + 1) * BLK)
            part = slice(h * BLK, (h + 1) * BLK)
            norm_old, curvature, crossing, square = (total[2 * n + h : 2 * n + h + 1] for n in range(4))
            step = norm_old / curvature
            norm_new = norm_old - 2.0 * step * crossing + step * step * square
            ratio = norm_new / norm_old
            product = jnp.where(mine, image[here, part], other[here, part])
            d = direction[here, lanes]
            sol_next[:, lanes] = solution[here, lanes] + step * d
            r = residual[here, lanes] - step * product
            res_next[:, lanes] = r
            dir_next[:, lanes] = r + ratio * d


def in_hbm(x):
    return pltpu.with_memory_space_constraint(x, pltpu.HBM)


def vmem(n):
    return [pl.BlockSpec(memory_space=pltpu.VMEM)] * n


def from_all(x, axes):
    return lax.all_to_all(x, axes, 0, 0, tiled=True)


def iteration(gain, coupled_columns, solution, residual, direction):
    rows, _ = gain.shape[:2]
    states, snapshots = direction.shape
    half = snapshots // 2
    groups = lax.axis_size(ROW_COL)

    halves = jax.ShapeDtypeStruct((states, half), F32)
    own = pl.pallas_call(
        take_half,
        out_shape=halves,
        in_specs=[pl.BlockSpec(memory_space=pltpu.HBM)],
        out_specs=vmem(1)[0],
        scratch_shapes=[pltpu.SemaphoreType.DMA],
        compiler_params=pltpu.CompilerParams(vmem_limit_bytes=2 << 20),
        name="take_half",
    )(in_hbm(direction))
    one = lax.ppermute(own, ALL, halo_pairs(groups, True))
    two = lax.ppermute(own, ALL, halo_pairs(groups, False))
    other_gain = lax.ppermute(gain, "rep", [(0, 1), (1, 0)])
    smem = pl.BlockSpec(memory_space=pltpu.SMEM)
    whole = jax.ShapeDtypeStruct((states, snapshots), F32)
    terms = jax.ShapeDtypeStruct((REACH, states, BLK), BF16)
    band = jax.ShapeDtypeStruct((3 * rows, states, BLK), F32)
    dense, norm, res, dir_, sol = pl.pallas_call(
        begin,
        out_shape=(band, jax.ShapeDtypeStruct((1, half), F32), whole, whole, whole),
        in_specs=[smem, *[pl.BlockSpec(memory_space=pltpu.HBM)] * 4],
        out_specs=tuple(vmem(5)),
        scratch_shapes=[pltpu.VMEM(gain.shape, F32), pltpu.SemaphoreType.DMA((4,))],
        cost_estimate=pl.CostEstimate(flops=4_000_000, bytes_accessed=5_000_000, transcendentals=0),
        compiler_params=pltpu.CompilerParams(vmem_limit_bytes=12 << 20),
        name="begin",
    )(in_hbm(coupled_columns), *map(in_hbm, (gain, residual, direction, solution)))
    *terms, local = pl.pallas_call(
        prepare,
        out_shape=(*[terms] * 4, halves),
        in_specs=[smem, *vmem(3)],
        out_specs=tuple(vmem(5)),
        scratch_shapes=[pltpu.VMEM(band.shape, F32)],
        cost_estimate=pl.CostEstimate(flops=400_000_000, bytes_accessed=5_000_000, transcendentals=0),
        compiler_params=pltpu.CompilerParams(vmem_limit_bytes=10 << 20),
        name="prepare",
    )(in_hbm(coupled_columns), other_gain, own, dense)

    n1 = lax.axis_size("row") * lax.axis_size("col_1")
    n2 = 2 * lax.axis_size("col_0")
    partial = pl.pallas_call(
        first_halo,
        out_shape=halves,
        in_specs=vmem(4),
        out_specs=vmem(1)[0],
        cost_estimate=pl.CostEstimate(flops=250_000_000, bytes_accessed=1_000_000, transcendentals=0),
        compiler_params=pltpu.CompilerParams(vmem_limit_bytes=8 << 20),
        name="first_halo",
    )(one, terms[0], terms[1], local)
    image, sums = pl.pallas_call(
        finish,
        out_shape=(halves, jax.ShapeDtypeStruct((n1, 8, BLK), F32)),
        in_specs=vmem(7),
        out_specs=tuple(vmem(2)),
        cost_estimate=pl.CostEstimate(flops=500_000_000, bytes_accessed=5_000_000, transcendentals=0),
        compiler_params=pltpu.CompilerParams(vmem_limit_bytes=10 << 20),
        name="finish",
    )(two, terms[2], terms[3], partial, own, res, norm)
    sums = from_all(sums, ("col_1", "row"))
    other_image = lax.ppermute(image, "rep", [(0, 1), (1, 0)])
    sums = pl.pallas_call(
        fold,
        out_shape=jax.ShapeDtypeStruct((n2, 8, BLK), F32),
        in_specs=vmem(1),
        out_specs=vmem(1)[0],
        compiler_params=pltpu.CompilerParams(vmem_limit_bytes=2 << 20),
        name="fold",
    )(sums)
    sums = from_all(sums, ("rep", "col_0"))

    chunk = states // CHUNKS
    block = pl.BlockSpec((chunk, snapshots), lambda c: (c, 0))
    return pl.pallas_call(
        update,
        grid=(CHUNKS,),
        out_shape=(whole, whole, whole),
        in_specs=vmem(6),
        out_specs=(block, block, block),
        compiler_params=pltpu.CompilerParams(vmem_limit_bytes=10 << 20),
        name="update",
    )(sums, image, other_image, sol, res, dir_)


def solution(mesh):
    finer = Mesh(
        mesh.devices.reshape(mesh.shape["row"], 8, 4, mesh.shape["rep"]),
        ALL,
    )
    return jax.shard_map(
        iteration,
        mesh=finer,
        in_specs=(
            P(ROW_COL, "rep", None, None),
            P(ROW_COL, None),
            P(ROW_COL, None),
            P(ROW_COL, None),
            P(ROW_COL, None),
        ),
        out_specs=(P(ROW_COL, None), P(ROW_COL, None), P(ROW_COL, None)),
        check_vma=False,
    )
```

```python
import jax
import jax.numpy as jnp
from jax import lax
from jax.experimental import pallas as pl
from jax.experimental.pallas import tpu as pltpu
from jax.sharding import Mesh
from jax.sharding import PartitionSpec as P

BLK = 128
REACH = 3
CHUNKS = 2
ROW_COL = ("row", "col_0", "col_1")
ALL = ("row", "col_0", "col_1", "rep")
F32, BF16 = jnp.float32, jnp.bfloat16


def halo_pairs(groups, first):
    pairs = []
    for rep in range(2):
        for p in range((rep + 1 - first) % 2, groups - 1, 2):
            near, far = 2 * p + rep, 2 * (p + 1) + rep
            pairs += [(near, far), (far, near)]
    return pairs


def split(x):
    top = x.astype(BF16)
    return top, (x - top.astype(F32)).astype(BF16)


def dot3(a_top, a_rest, x):
    x_top, x_rest = split(x)
    dot = lambda a, b: jnp.dot(a, b, preferred_element_type=F32)
    return dot(a_top, x_top) + (dot(a_top, x_rest) + dot(a_rest, x_top))


def take_half(direction, own, sem):
    half = own.shape[1]
    at = pl.ds(pl.multiple_of(lax.axis_index("rep") * half, half), half)
    copy = pltpu.make_async_copy(direction.at[:, at], own, sem)
    copy.start()
    copy.wait()


def place_blocks(columns, blocks, offset, dense):
    rows, slots = blocks.shape[0], blocks.shape[1]
    segment = lax.axis_index(ROW_COL)
    low_first = (segment + lax.axis_index("rep")) % 2 == 1
    for i in range(rows):
        for k in range(slots):
            w = columns[i, offset + k] - segment * rows + REACH
            low = jnp.where(low_first, w, w + 3)
            high = jnp.where(low_first, w - 3, w - 6)
            c = jnp.where(w < 3, low, jnp.where(w > 5, high, w + 3))
            here = pl.ds(i * BLK, BLK)
            dense[c, here, :] = dense[c, here, :] + blocks[i, k]


def begin(columns, gain, residual, direction, solution, dense, norm, res, dir_, sol, mine, sems):
    rep = lax.axis_index("rep")
    half = residual.shape[1] // 2
    ends = ((gain, mine), (residual, res), (direction, dir_), (solution, sol))
    copies = [pltpu.make_async_copy(*pair, sems.at[n]) for n, pair in enumerate(ends)]
    for copy in copies:
        copy.start()
    dense[...] = jnp.zeros_like(dense)
    copies[0].wait()
    place_blocks(columns, mine, rep * mine.shape[1], dense)
    copies[1].wait()
    r = res[:, pl.ds(pl.multiple_of(rep * half, half), half)]
    norm[...] = jnp.sum(r * r, axis=0, keepdims=True)
    copies[2].wait()
    copies[3].wait()


def prepare(columns, other, own, start, top_1, rest_1, top_2, rest_2, local, dense):
    dense[...] = start[...]
    place_blocks(columns, other, (1 - lax.axis_index("rep")) * other.shape[1], dense)
    for c in range(3):
        top_1[c], rest_1[c] = split(dense[c])
        top_2[c], rest_2[c] = split(dense[3 + c])
    middle = jnp.concatenate([dense[6], dense[7], dense[8]], axis=1)
    m_top, m_rest = split(middle)
    local[...] = dot3(m_top, m_rest, own[...])


def add_halo(start, x, top, rest):
    join = lambda terms: jnp.concatenate([terms[c] for c in range(3)], axis=1)
    return start[...] + dot3(join(top), join(rest), x[...])


def first_halo(one, top, rest, local, partial):
    partial[...] = add_halo(local, one, top, rest)


def finish(two, top, rest, partial, own, res, norm, image, sums):
    product = add_halo(partial, two, top, rest)
    half = product.shape[1]
    image[...] = product
    r = res[:, pl.ds(pl.multiple_of(lax.axis_index("rep") * half, half), half)]
    rows = [
        norm[...],
        jnp.sum(own[...] * product, axis=0, keepdims=True),
        jnp.sum(r * product, axis=0, keepdims=True),
        jnp.sum(product * product, axis=0, keepdims=True),
    ]
    packed = jnp.concatenate([v[:, h : h + BLK] for v in rows for h in range(0, half, BLK)], axis=0)
    sums[...] = jnp.broadcast_to(packed[None], sums.shape)


def fold(terms, sums):
    sums[...] = jnp.broadcast_to(jnp.sum(terms[...], axis=0)[None], sums.shape)


def update(terms, image, other, solution, residual, direction, sol_next, res_next, dir_next):
    half = image.shape[1]
    chunk = sol_next.shape[0]
    rep = lax.axis_index("rep")
    here = pl.ds(pl.multiple_of(pl.program_id(0) * chunk, chunk), chunk)
    for side in range(2):
        count = terms.shape[0] // 2
        total = terms[side * count]
        for n in range(1, count):
            total += terms[side * count + n]
        mine = rep == side
        for h in range(half // BLK):
            lanes = slice(side * half + h * BLK, side * half + (h + 1) * BLK)
            part = slice(h * BLK, (h + 1) * BLK)
            norm_old, curvature, crossing, square = (total[2 * n + h : 2 * n + h + 1] for n in range(4))
            step = norm_old / curvature
            norm_new = norm_old - 2.0 * step * crossing + step * step * square
            ratio = norm_new / norm_old
            product = jnp.where(mine, image[here, part], other[here, part])
            d = direction[here, lanes]
            sol_next[:, lanes] = solution[here, lanes] + step * d
            r = residual[here, lanes] - step * product
            res_next[:, lanes] = r
            dir_next[:, lanes] = r + ratio * d


def in_hbm(x):
    return pltpu.with_memory_space_constraint(x, pltpu.HBM)


def vmem(n):
    return [pl.BlockSpec(memory_space=pltpu.VMEM)] * n


def from_all(x, axes):
    return lax.all_to_all(x, axes, 0, 0, tiled=True)


def iteration(gain, coupled_columns, solution, residual, direction):
    rows, _ = gain.shape[:2]
    states, snapshots = direction.shape
    half = snapshots // 2
    groups = lax.axis_size(ROW_COL)

    halves = jax.ShapeDtypeStruct((states, half), F32)
    own = pl.pallas_call(
        take_half,
        out_shape=halves,
        in_specs=[pl.BlockSpec(memory_space=pltpu.HBM)],
        out_specs=vmem(1)[0],
        scratch_shapes=[pltpu.SemaphoreType.DMA],
        compiler_params=pltpu.CompilerParams(vmem_limit_bytes=2 << 20),
        name="take_half",
    )(in_hbm(direction))
    one = lax.ppermute(own, ALL, halo_pairs(groups, True))
    two = lax.ppermute(own, ALL, halo_pairs(groups, False))
    other_gain = lax.ppermute(gain, "rep", [(0, 1), (1, 0)])
    smem = pl.BlockSpec(memory_space=pltpu.SMEM)
    whole = jax.ShapeDtypeStruct((states, snapshots), F32)
    terms = jax.ShapeDtypeStruct((REACH, states, BLK), BF16)
    band = jax.ShapeDtypeStruct((3 * rows, states, BLK), F32)
    dense, norm, res, dir_, sol = pl.pallas_call(
        begin,
        out_shape=(band, jax.ShapeDtypeStruct((1, half), F32), whole, whole, whole),
        in_specs=[smem, *[pl.BlockSpec(memory_space=pltpu.HBM)] * 4],
        out_specs=tuple(vmem(5)),
        scratch_shapes=[pltpu.VMEM(gain.shape, F32), pltpu.SemaphoreType.DMA((4,))],
        cost_estimate=pl.CostEstimate(flops=4_000_000, bytes_accessed=5_000_000, transcendentals=0),
        compiler_params=pltpu.CompilerParams(vmem_limit_bytes=12 << 20),
        name="begin",
    )(in_hbm(coupled_columns), *map(in_hbm, (gain, residual, direction, solution)))
    *terms, local = pl.pallas_call(
        prepare,
        out_shape=(*[terms] * 4, halves),
        in_specs=[smem, *vmem(3)],
        out_specs=tuple(vmem(5)),
        scratch_shapes=[pltpu.VMEM(band.shape, F32)],
        cost_estimate=pl.CostEstimate(flops=400_000_000, bytes_accessed=5_000_000, transcendentals=0),
        compiler_params=pltpu.CompilerParams(vmem_limit_bytes=10 << 20),
        name="prepare",
    )(in_hbm(coupled_columns), other_gain, own, dense)

    n1 = lax.axis_size("col_0") * lax.axis_size("col_1")
    n2 = 2 * lax.axis_size("row")
    partial = pl.pallas_call(
        first_halo,
        out_shape=halves,
        in_specs=vmem(4),
        out_specs=vmem(1)[0],
        cost_estimate=pl.CostEstimate(flops=250_000_000, bytes_accessed=1_000_000, transcendentals=0),
        compiler_params=pltpu.CompilerParams(vmem_limit_bytes=8 << 20),
        name="first_halo",
    )(one, terms[0], terms[1], local)
    image, sums = pl.pallas_call(
        finish,
        out_shape=(halves, jax.ShapeDtypeStruct((n1, 8, BLK), F32)),
        in_specs=vmem(7),
        out_specs=tuple(vmem(2)),
        cost_estimate=pl.CostEstimate(flops=500_000_000, bytes_accessed=5_000_000, transcendentals=0),
        compiler_params=pltpu.CompilerParams(vmem_limit_bytes=10 << 20),
        name="finish",
    )(two, terms[2], terms[3], partial, own, res, norm)
    sums = from_all(sums, ("col_1", "col_0"))
    other_image = lax.ppermute(image, "rep", [(0, 1), (1, 0)])
    sums = pl.pallas_call(
        fold,
        out_shape=jax.ShapeDtypeStruct((n2, 8, BLK), F32),
        in_specs=vmem(1),
        out_specs=vmem(1)[0],
        compiler_params=pltpu.CompilerParams(vmem_limit_bytes=2 << 20),
        name="fold",
    )(sums)
    sums = from_all(sums, ("rep", "row"))

    chunk = states // CHUNKS
    block = pl.BlockSpec((chunk, snapshots), lambda c: (c, 0))
    return pl.pallas_call(
        update,
        grid=(CHUNKS,),
        out_shape=(whole, whole, whole),
        in_specs=vmem(6),
        out_specs=(block, block, block),
        compiler_params=pltpu.CompilerParams(vmem_limit_bytes=10 << 20),
        name="update",
    )(sums, image, other_image, sol, res, dir_)


def solution(mesh):
    finer = Mesh(
        mesh.devices.reshape(mesh.shape["row"], 8, 4, mesh.shape["rep"]),
        ALL,
    )
    return jax.shard_map(
        iteration,
        mesh=finer,
        in_specs=(
            P(ROW_COL, "rep", None, None),
            P(ROW_COL, None),
            P(ROW_COL, None),
            P(ROW_COL, None),
            P(ROW_COL, None),
        ),
        out_specs=(P(ROW_COL, None), P(ROW_COL, None), P(ROW_COL, None)),
        check_vma=False,
    )
```

```python
import jax
import jax.numpy as jnp
from jax import lax
from jax.experimental import pallas as pl
from jax.experimental.pallas import tpu as pltpu
from jax.sharding import Mesh
from jax.sharding import PartitionSpec as P

BLK = 128
REACH = 3
CHUNKS = 2
ROW_COL = ("row", "col_0", "col_1")
ALL = ("row", "col_0", "col_1", "rep")
F32, BF16 = jnp.float32, jnp.bfloat16


def halo_pairs(groups, first):
    step = 1 if first else -1
    pairs = []
    for p in range(groups):
        for rep, to in ((0, p + step), (1, p - step)):
            if 0 <= to < groups:
                pairs.append((2 * p + rep, 2 * to + rep))
    return pairs


def split(x):
    top = x.astype(BF16)
    return top, (x - top.astype(F32)).astype(BF16)


def dot3(a_top, a_rest, x):
    x_top, x_rest = split(x)
    dot = lambda a, b: jnp.dot(a, b, preferred_element_type=F32)
    return dot(a_top, x_top) + (dot(a_top, x_rest) + dot(a_rest, x_top))


def take_half(direction, own, sem):
    half = own.shape[1]
    at = pl.ds(pl.multiple_of(lax.axis_index("rep") * half, half), half)
    copy = pltpu.make_async_copy(direction.at[:, at], own, sem)
    copy.start()
    copy.wait()


def place_blocks(columns, blocks, offset, dense):
    rows, slots = blocks.shape[0], blocks.shape[1]
    segment = lax.axis_index(ROW_COL)
    low_first = lax.axis_index("rep") == 0
    for i in range(rows):
        for k in range(slots):
            w = columns[i, offset + k] - segment * rows + REACH
            low = jnp.where(low_first, w, w + 3)
            high = jnp.where(low_first, w - 3, w - 6)
            c = jnp.where(w < 3, low, jnp.where(w > 5, high, w + 3))
            here = pl.ds(i * BLK, BLK)
            dense[c, here, :] = dense[c, here, :] + blocks[i, k]


def begin(columns, gain, residual, direction, solution, dense, norm, res, dir_, sol, mine, sems):
    rep = lax.axis_index("rep")
    half = residual.shape[1] // 2
    ends = ((gain, mine), (residual, res), (direction, dir_), (solution, sol))
    copies = [pltpu.make_async_copy(*pair, sems.at[n]) for n, pair in enumerate(ends)]
    for copy in copies:
        copy.start()
    dense[...] = jnp.zeros_like(dense)
    copies[0].wait()
    place_blocks(columns, mine, rep * mine.shape[1], dense)
    copies[1].wait()
    r = res[:, pl.ds(pl.multiple_of(rep * half, half), half)]
    norm[...] = jnp.sum(r * r, axis=0, keepdims=True)
    copies[2].wait()
    copies[3].wait()


def prepare(columns, other, own, start, top_1, rest_1, top_2, rest_2, local, dense):
    dense[...] = start[...]
    place_blocks(columns, other, (1 - lax.axis_index("rep")) * other.shape[1], dense)
    for c in range(3):
        top_1[c], rest_1[c] = split(dense[c])
        top_2[c], rest_2[c] = split(dense[3 + c])
    middle = jnp.concatenate([dense[6], dense[7], dense[8]], axis=1)
    m_top, m_rest = split(middle)
    local[...] = dot3(m_top, m_rest, own[...])


def add_halo(start, x, top, rest):
    join = lambda terms: jnp.concatenate([terms[c] for c in range(3)], axis=1)
    return start[...] + dot3(join(top), join(rest), x[...])


def first_halo(one, top, rest, local, partial):
    partial[...] = add_halo(local, one, top, rest)


def finish(two, top, rest, partial, own, res, norm, image, sums):
    product = add_halo(partial, two, top, rest)
    half = product.shape[1]
    image[...] = product
    r = res[:, pl.ds(pl.multiple_of(lax.axis_index("rep") * half, half), half)]
    rows = [
        norm[...],
        jnp.sum(own[...] * product, axis=0, keepdims=True),
        jnp.sum(r * product, axis=0, keepdims=True),
        jnp.sum(product * product, axis=0, keepdims=True),
    ]
    packed = jnp.concatenate([v[:, h : h + BLK] for v in rows for h in range(0, half, BLK)], axis=0)
    sums[...] = jnp.broadcast_to(packed[None], sums.shape)


def fold(terms, sums):
    sums[...] = jnp.broadcast_to(jnp.sum(terms[...], axis=0)[None], sums.shape)


def update(terms, image, other, solution, residual, direction, sol_next, res_next, dir_next):
    half = image.shape[1]
    chunk = sol_next.shape[0]
    rep = lax.axis_index("rep")
    here = pl.ds(pl.multiple_of(pl.program_id(0) * chunk, chunk), chunk)
    for side in range(2):
        count = terms.shape[0] // 2
        total = terms[side * count]
        for n in range(1, count):
            total += terms[side * count + n]
        mine = rep == side
        for h in range(half // BLK):
            lanes = slice(side * half + h * BLK, side * half + (h + 1) * BLK)
            part = slice(h * BLK, (h + 1) * BLK)
            norm_old, curvature, crossing, square = (total[2 * n + h : 2 * n + h + 1] for n in range(4))
            step = norm_old / curvature
            norm_new = norm_old - 2.0 * step * crossing + step * step * square
            ratio = norm_new / norm_old
            product = jnp.where(mine, image[here, part], other[here, part])
            d = direction[here, lanes]
            sol_next[:, lanes] = solution[here, lanes] + step * d
            r = residual[here, lanes] - step * product
            res_next[:, lanes] = r
            dir_next[:, lanes] = r + ratio * d


def in_hbm(x):
    return pltpu.with_memory_space_constraint(x, pltpu.HBM)


def vmem(n):
    return [pl.BlockSpec(memory_space=pltpu.VMEM)] * n


def from_all(x, axes):
    return lax.all_to_all(x, axes, 0, 0, tiled=True)


def iteration(gain, coupled_columns, solution, residual, direction):
    rows, _ = gain.shape[:2]
    states, snapshots = direction.shape
    half = snapshots // 2
    groups = lax.axis_size(ROW_COL)

    halves = jax.ShapeDtypeStruct((states, half), F32)
    own = pl.pallas_call(
        take_half,
        out_shape=halves,
        in_specs=[pl.BlockSpec(memory_space=pltpu.HBM)],
        out_specs=vmem(1)[0],
        scratch_shapes=[pltpu.SemaphoreType.DMA],
        compiler_params=pltpu.CompilerParams(vmem_limit_bytes=2 << 20),
        name="take_half",
    )(in_hbm(direction))
    one = lax.ppermute(own, ALL, halo_pairs(groups, True))
    two = lax.ppermute(own, ALL, halo_pairs(groups, False))
    other_gain = lax.ppermute(gain, "rep", [(0, 1), (1, 0)])
    smem = pl.BlockSpec(memory_space=pltpu.SMEM)
    whole = jax.ShapeDtypeStruct((states, snapshots), F32)
    terms = jax.ShapeDtypeStruct((REACH, states, BLK), BF16)
    band = jax.ShapeDtypeStruct((3 * rows, states, BLK), F32)
    dense, norm, res, dir_, sol = pl.pallas_call(
        begin,
        out_shape=(band, jax.ShapeDtypeStruct((1, half), F32), whole, whole, whole),
        in_specs=[smem, *[pl.BlockSpec(memory_space=pltpu.HBM)] * 4],
        out_specs=tuple(vmem(5)),
        scratch_shapes=[pltpu.VMEM(gain.shape, F32), pltpu.SemaphoreType.DMA((4,))],
        cost_estimate=pl.CostEstimate(flops=4_000_000, bytes_accessed=5_000_000, transcendentals=0),
        compiler_params=pltpu.CompilerParams(vmem_limit_bytes=12 << 20),
        name="begin",
    )(in_hbm(coupled_columns), *map(in_hbm, (gain, residual, direction, solution)))
    *terms, local = pl.pallas_call(
        prepare,
        out_shape=(*[terms] * 4, halves),
        in_specs=[smem, *vmem(3)],
        out_specs=tuple(vmem(5)),
        scratch_shapes=[pltpu.VMEM(band.shape, F32)],
        cost_estimate=pl.CostEstimate(flops=400_000_000, bytes_accessed=5_000_000, transcendentals=0),
        compiler_params=pltpu.CompilerParams(vmem_limit_bytes=10 << 20),
        name="prepare",
    )(in_hbm(coupled_columns), other_gain, own, dense)

    n1 = lax.axis_size("col_0") * lax.axis_size("col_1")
    n2 = 2 * lax.axis_size("row")
    partial = pl.pallas_call(
        first_halo,
        out_shape=halves,
        in_specs=vmem(4),
        out_specs=vmem(1)[0],
        cost_estimate=pl.CostEstimate(flops=250_000_000, bytes_accessed=1_000_000, transcendentals=0),
        compiler_params=pltpu.CompilerParams(vmem_limit_bytes=8 << 20),
        name="first_halo",
    )(one, terms[0], terms[1], local)
    image, sums = pl.pallas_call(
        finish,
        out_shape=(halves, jax.ShapeDtypeStruct((n1, 8, BLK), F32)),
        in_specs=vmem(7),
        out_specs=tuple(vmem(2)),
        cost_estimate=pl.CostEstimate(flops=500_000_000, bytes_accessed=5_000_000, transcendentals=0),
        compiler_params=pltpu.CompilerParams(vmem_limit_bytes=10 << 20),
        name="finish",
    )(two, terms[2], terms[3], partial, own, res, norm)
    sums = from_all(sums, ("col_1", "col_0"))
    other_image = lax.ppermute(image, "rep", [(0, 1), (1, 0)])
    sums = pl.pallas_call(
        fold,
        out_shape=jax.ShapeDtypeStruct((n2, 8, BLK), F32),
        in_specs=vmem(1),
        out_specs=vmem(1)[0],
        compiler_params=pltpu.CompilerParams(vmem_limit_bytes=2 << 20),
        name="fold",
    )(sums)
    sums = from_all(sums, ("rep", "row"))

    chunk = states // CHUNKS
    block = pl.BlockSpec((chunk, snapshots), lambda c: (c, 0))
    return pl.pallas_call(
        update,
        grid=(CHUNKS,),
        out_shape=(whole, whole, whole),
        in_specs=vmem(6),
        out_specs=(block, block, block),
        compiler_params=pltpu.CompilerParams(vmem_limit_bytes=10 << 20),
        name="update",
    )(sums, image, other_image, sol, res, dir_)


def solution(mesh):
    finer = Mesh(
        mesh.devices.reshape(mesh.shape["row"], 8, 4, mesh.shape["rep"]),
        ALL,
    )
    return jax.shard_map(
        iteration,
        mesh=finer,
        in_specs=(
            P(ROW_COL, "rep", None, None),
            P(ROW_COL, None),
            P(ROW_COL, None),
            P(ROW_COL, None),
            P(ROW_COL, None),
        ),
        out_specs=(P(ROW_COL, None), P(ROW_COL, None), P(ROW_COL, None)),
        check_vma=False,
    )
```
